32 devices in a mesh: seq: 16 (over z, y, core), fsdp: 2 (over x).
Axes of the slice: x: 2, y: 2, z: 4, core: 2. Of those that a mesh axis runs over, the one named last changes fastest.
Arguments:
- tokens: bfloat16 [64, 8192], P('seq', 'fsdp'), may hold values from -6 to 6
- gate_weight: bfloat16 [8192, 16384], P('fsdp', 'seq'), may hold values from -0.0625 to 0.0625
- up_weight: bfloat16 [8192, 16384], P('fsdp', 'seq'), may hold values from -0.0625 to 0.0625
- down_weight: bfloat16 [8192, 16384], P('fsdp', 'seq'), may hold values from -0.046875 to 0.046875
Outputs:
- mixed_out: bfloat16 [64, 8192], P('seq', 'fsdp')
The draws below stay inside these ranges and needn't reach their ends.
All inputs are finite; a program needn't handle non-finite values.
Results may differ from the reference program's by a relative error of at most 0.0049.
Values may be sent and summed in bfloat16 or wider, within the bound.
A program may use at most 64 MiB of HBM per device.

```python
import jax
import jax.numpy as jnp
from jax import lax

D = 8192
FF = 16384
TOKENS = 64


def level_of(key, shape, split, low, top_value):
    def one(dim, parts):
        draws = jax.random.uniform(jax.random.fold_in(jax.random.fold_in(key, 6), dim), (parts,), jnp.float32, low / len(split), top_value / len(split))
        return jnp.repeat(jnp.exp(draws), shape[dim] // parts).reshape((-1,) + (1,) * (len(shape) - dim - 1))

    gain = one(*split[0])
    for cut in split[1:]:
        gain = gain * one(*cut)
    return gain


def scatter_about(rng, extent, spread, limit, shards=(), dtype=jnp.bfloat16):
    gain = level_of(rng, extent, shards, -0.22, 0.18) if shards else 1.0
    entries = jax.random.normal(rng, extent, jnp.float32) * spread * gain
    return jnp.minimum(jnp.maximum(entries, -limit), limit).astype(dtype)


def setup_inputs(seed: int = 0) -> dict:
    streams_of = jax.random.split(jax.random.key(seed), 5)
    return {
        "tokens": scatter_about(streams_of[0], (TOKENS, D), 1.0, 6.0, ((0, 16), (1, 2))),
        "gate_weight": scatter_about(streams_of[1], (D, FF), D ** -0.5, 0.0625, ((0, 2), (1, 16))),
        "up_weight": scatter_about(streams_of[2], (D, FF), D ** -0.5, 0.0625, ((0, 2), (1, 16))),
        "down_weight": scatter_about(streams_of[3], (D, FF), FF ** -0.5, 0.046875, ((0, 2), (1, 16))),
    }


def project_down(hidden, weight):
    return lax.dot_general(hidden, weight, (((1,), (1,)), ((), ())), preferred_element_type=jnp.float32)


def reference(tokens, gate_weight, up_weight, down_weight):
    gate_value = jnp.dot(tokens, gate_weight, preferred_element_type=jnp.float32)
    up_value = jnp.dot(tokens, up_weight, preferred_element_type=jnp.float32)
    hidden = (jax.nn.silu(gate_value) * up_value).astype(jnp.bfloat16)
    return project_down(hidden, down_weight).astype(jnp.bfloat16)
```

```python
import functools

import jax
import jax.numpy as jnp
from jax import lax
from jax.experimental import pallas as pl
from jax.experimental.pallas import tpu as pltpu
from jax.sharding import PartitionSpec as P

MESH = pl.DeviceIdType.MESH
F32, BF16 = jnp.float32, jnp.bfloat16
KC, FC = 2, 4


def ffn(R, T, UC, tok, wg, wu, wd, out, G, X, VG, VU, VD, A, SX, RX, H, O, RC, SY, RY,
        S2, SZ, RZ, wsem, dsem, tsem, gz, gy, gc, gr, xs, xr, cs, cr, ys, yr, zs, zr):
    idx, x = lax.axis_index("seq"), lax.axis_index("fsdp")
    c, y, r = lax.rem(idx, 2), lax.rem(lax.div(idx, 2), 2), lax.div(idx, 4)
    core_peer = (idx + 1 - 2 * c, x)
    y_peer = (idx + 2 - 4 * y, x)
    x_peer = (idx, 1 - x)
    away = [lax.rem(r + d, R) for d in range(R)]
    z_peer = [(rr * 4 + y * 2 + c, x) for rr in away]
    kw, fw, uw = G.shape[-1], O.shape[-1], SX.shape[-1]
    rows = X.shape[1]
    mine = R * T

    toks = [pltpu.make_async_copy(tok.at[:, pl.ds(k * kw, kw)], G.at[k, c, y, r], tsem.at[k]) for k in range(KC)]
    for t in toks:
        t.start()
    weights = []
    for k in range(KC):
        part = pl.ds(k * kw, kw)
        weights.append([pltpu.make_async_copy(w.at[part], v.at[part], wsem.at[i, k]) for i, (w, v) in enumerate(((wg, VG), (wu, VU)))])
        for w in weights[-1]:
            w.start()
    downs = []
    for f in range(FC):
        part = pl.ds(f * fw, fw)
        downs.append(pltpu.make_async_copy(wd.at[part], VD.at[part], dsem.at[f]))
        downs[-1].start()

    barrier = pltpu.get_barrier_semaphore()
    peers = z_peer[1:] + [y_peer, core_peer, x_peer]
    for p in peers:
        pl.semaphore_signal(barrier, inc=1, device_id=p, device_id_type=MESH)
    pl.semaphore_wait(barrier, len(peers))

    sent = []

    def send(src, dst, s, q, peer):
        copy = pltpu.make_async_remote_copy(src_ref=src, dst_ref=dst, send_sem=s, recv_sem=q, device_id=peer, device_id_type=MESH)
        copy.start()
        sent.append(copy)

    def await_block(k, cc, yy, rr):
        g = G.at[k, cc, yy, rr]
        pltpu.make_async_remote_copy(src_ref=g, dst_ref=g, send_sem=gz.at[k, 0], recv_sem=gr.at[k, cc, yy, rr],
                                     device_id=core_peer, device_id_type=MESH).wait_recv()

    def to_peer(k, yy, rr, s, peer):
        g = G.at[k, c, yy, rr]
        send(g, g, s, gr.at[k, c, yy, rr], peer)

    for k in range(KC):
        toks[k].wait()
        for d in range(1, R):
            to_peer(k, y, r, gz.at[k, d], z_peer[d])
        to_peer(k, y, r, gy.at[k, 0], y_peer)
        to_peer(k, y, r, gc.at[k, 0, 0], core_peer)
    for k in range(KC):
        for d in range(1, R):
            await_block(k, c, y, away[d])
            to_peer(k, y, away[d], gy.at[k, d], y_peer)
            to_peer(k, y, away[d], gc.at[k, 0, d], core_peer)
    for k in range(KC):
        for d in range(R):
            await_block(k, c, 1 - y, away[d])
            to_peer(k, 1 - y, away[d], gc.at[k, 1, d], core_peer)
    for k in range(KC):
        for yy in (y, 1 - y):
            for d in range(R):
                await_block(k, 1 - c, yy, away[d])
        for cc in range(2):
            for yy in range(2):
                at = (cc * 2 + yy) * mine
                X[k, at:at + mine, :] = G[k, cc, yy].reshape(mine, kw)
        for w in weights[k]:
            w.wait()
        for u in range(UC):
            cols = pl.ds(u * uw, uw)
            for i, v in enumerate((VG, VU)):
                value = jnp.dot(X[k], v[pl.ds(k * kw, kw), cols], preferred_element_type=F32)
                if k > 0:
                    value += A[i, :, cols]
                A[i, :, cols] = value
                if k == KC - 1:
                    SX[u, i] = value.astype(BF16)
            if k == KC - 1:
                send(SX.at[u], RX.at[u], xs.at[u], xr.at[u], x_peer)

    def await_x(u):
        pltpu.make_async_remote_copy(src_ref=SX.at[u], dst_ref=RX.at[u], send_sem=xs.at[u], recv_sem=xr.at[u],
                                     device_id=x_peer, device_id_type=MESH).wait_recv()

    def down(f, lo, hi):
        return lax.dot_general(H[:, lo:hi], VD[pl.ds(f * fw, fw), lo:hi], (((1,), (1,)), ((), ())),
                               preferred_element_type=F32).reshape(2, 2, mine, fw)

    def hidden(u):
        await_x(u)
        cols = pl.ds(u * uw, uw)
        gate = A[0, :, cols] + RX[u, 0].astype(F32)
        up = A[1, :, cols] + RX[u, 1].astype(F32)
        H[:, cols] = (gate / (1.0 + jnp.exp(-gate)) * up).astype(BF16)

    half = UC // 2
    for u in range(half):
        hidden(u)
    for f in range(FC):
        downs[f].wait()
        if half:
            O[f] = down(f, 0, half * uw)
    for u in range(half, UC):
        hidden(u)

    arrivals = {}

    def to_core(f):
        value = down(f, half * uw, UC * uw)
        O[f] = O[f] + value if half else value
        send(O.at[f, 1 - c], RC.at[f], cs.at[f], cr.at[f], core_peer)
        arrivals["c", f] = sent[-1]

    def to_y(f):
        arrivals["c", f].wait_recv()
        SY[f] = (O[f, c, 1 - y] + RC[f, 1 - y]).astype(BF16)
        send(SY.at[f], RY.at[f], ys.at[f], yr.at[f], y_peer)
        arrivals["y", f] = sent[-1]

    def to_z(f):
        arrivals["y", f].wait_recv()
        total = (O[f, c, y] + RC[f, y] + RY[f].astype(F32)).reshape(R, T, fw)
        S2[f] = total
        SZ[f] = total.astype(BF16)
        for d in range(1, R):
            send(SZ.at[f, away[d]], RZ.at[f, d], zs.at[f, d], zr.at[f, d], z_peer[d])
            arrivals["z", f, d] = sent[-1]

    def finish(f):
        total = S2[f, r]
        for d in range(1, R):
            arrivals["z", f, d].wait_recv()
            total += RZ[f, d].astype(F32)
        out[:, pl.ds(f * fw, fw)] = total.astype(BF16)

    for f in range(FC):
        to_core(f)
        if f:
            to_y(f - 1)
    to_y(FC - 1)
    for f in range(FC):
        to_z(f)
    for f in range(FC):
        finish(f)
    for copy in sent:
        copy.wait_send()


def solution(mesh):
    n = mesh.shape["seq"]

    def on_device(tok, wg, wu, wd):
        T, K = tok.shape
        U = wg.shape[1]
        F = wd.shape[0]
        R = n // 4
        UC = max(1, U // 256)
        uw, kw, fw, rows, mine = U // UC, K // KC, F // FC, n * T, R * T
        dma = pltpu.SemaphoreType.DMA
        scratch = [
            pltpu.VMEM((KC, 2, 2, R, T, kw), BF16),
            pltpu.VMEM((KC, rows, kw), BF16),
            pltpu.VMEM((K, U), BF16),
            pltpu.VMEM((K, U), BF16),
            pltpu.VMEM((F, U), BF16),
            pltpu.VMEM((2, rows, U), F32),
            pltpu.VMEM((UC, 2, rows, uw), BF16),
            pltpu.VMEM((UC, 2, rows, uw), BF16),
            pltpu.VMEM((rows, U), BF16),
            pltpu.VMEM((FC, 2, 2, mine, fw), F32),
            pltpu.VMEM((FC, 2, mine, fw), F32),
            pltpu.VMEM((FC, mine, fw), BF16),
            pltpu.VMEM((FC, mine, fw), BF16),
            pltpu.VMEM((FC, R, T, fw), F32),
            pltpu.VMEM((FC, R, T, fw), BF16),
            pltpu.VMEM((FC, R, T, fw), BF16),
            dma((2, KC)), dma((FC,)), dma((KC,)),
            dma((KC, R)), dma((KC, R)), dma((KC, 2, R)), dma((KC, 2, 2, R)),
            dma((UC,)), dma((UC,)),
            dma((FC,)), dma((FC,)), dma((FC,)), dma((FC,)), dma((FC, R)), dma((FC, R)),
        ]
        return pl.pallas_call(
            functools.partial(ffn, R, T, UC),
            out_shape=jax.ShapeDtypeStruct((T, F), BF16),
            in_specs=[pl.BlockSpec(memory_space=pl.ANY)] * 4,
            out_specs=pl.BlockSpec(memory_space=pltpu.VMEM),
            scratch_shapes=scratch,
            compiler_params=pltpu.CompilerParams(
                collective_id=0, has_side_effects=True, vmem_limit_bytes=60 * 1024 * 1024
            ),
        )(tok, wg, wu, wd)

    return jax.shard_map(
        on_device,
        mesh=mesh,
        in_specs=(P("seq", "fsdp"), P("fsdp", "seq"), P("fsdp", "seq"), P("fsdp", "seq")),
        out_specs=P("seq", "fsdp"),
        check_vma=False,
    )
```

```python
import functools

import jax
import jax.numpy as jnp
from jax import lax
from jax.experimental import pallas as pl
from jax.experimental.pallas import tpu as pltpu
from jax.sharding import PartitionSpec as P

MESH = pl.DeviceIdType.MESH
F32, BF16 = jnp.float32, jnp.bfloat16
KC, FC = 4, 4


def ffn(R, T, UC, tok, wg, wu, wd, out, G, X, VG, VU, VD, A, SX, RX, H, O, RC, SY, RY,
        S2, SZ, RZ, wsem, dsem, tsem, gz, gy, gc, gr, xs, xr, cs, cr, ys, yr, zs, zr):
    idx, x = lax.axis_index("seq"), lax.axis_index("fsdp")
    c, y, r = lax.rem(idx, 2), lax.rem(lax.div(idx, 2), 2), lax.div(idx, 4)
    core_peer = (idx + 1 - 2 * c, x)
    y_peer = (idx + 2 - 4 * y, x)
    x_peer = (idx, 1 - x)
    away = [lax.rem(r + d, R) for d in range(R)]
    z_peer = [(rr * 4 + y * 2 + c, x) for rr in away]
    kw, fw, uw = G.shape[-1], O.shape[-1], SX.shape[-1]
    rows = X.shape[1]
    mine = R * T

    toks = [pltpu.make_async_copy(tok.at[:, pl.ds(k * kw, kw)], G.at[k, c, y, r], tsem.at[k]) for k in range(KC)]
    for t in toks:
        t.start()
    barrier = pltpu.get_barrier_semaphore()
    peers = z_peer[1:] + [y_peer, core_peer, x_peer]
    for p in peers:
        pl.semaphore_signal(barrier, inc=1, device_id=p, device_id_type=MESH)
    pl.semaphore_wait(barrier, len(peers))

    sent = []

    def send(src, dst, s, q, peer):
        copy = pltpu.make_async_remote_copy(src_ref=src, dst_ref=dst, send_sem=s, recv_sem=q, device_id=peer, device_id_type=MESH)
        copy.start()
        sent.append(copy)

    def await_block(k, cc, yy, rr):
        g = G.at[k, cc, yy, rr]
        pltpu.make_async_remote_copy(src_ref=g, dst_ref=g, send_sem=gz.at[k, 0], recv_sem=gr.at[k, cc, yy, rr],
                                     device_id=core_peer, device_id_type=MESH).wait_recv()

    def to_peer(k, yy, rr, s, peer):
        g = G.at[k, c, yy, rr]
        send(g, g, s, gr.at[k, c, yy, rr], peer)

    for k in range(KC):
        toks[k].wait()
        for d in range(1, R):
            to_peer(k, y, r, gz.at[k, d], z_peer[d])
        to_peer(k, y, r, gy.at[k, 0], y_peer)
        to_peer(k, y, r, gc.at[k, 0, 0], core_peer)
    weights = []
    for k in range(KC):
        part = pl.ds(k * kw, kw)
        weights.append([pltpu.make_async_copy(w.at[part], v.at[part], wsem.at[i, k]) for i, (w, v) in enumerate(((wg, VG), (wu, VU)))])
        for w in weights[-1]:
            w.start()
    downs = []
    for f in range(FC):
        part = pl.ds(f * fw, fw)
        downs.append(pltpu.make_async_copy(wd.at[part], VD.at[part], dsem.at[f]))
        downs[-1].start()

    for k in range(KC):
        for d in range(1, R):
            await_block(k, c, y, away[d])
            to_peer(k, y, away[d], gy.at[k, d], y_peer)
            to_peer(k, y, away[d], gc.at[k, 0, d], core_peer)
    for k in range(KC):
        for d in range(R):
            await_block(k, c, 1 - y, away[d])
            to_peer(k, 1 - y, away[d], gc.at[k, 1, d], core_peer)
    for k in range(KC):
        for yy in (y, 1 - y):
            for d in range(R):
                await_block(k, 1 - c, yy, away[d])
        for cc in range(2):
            for yy in range(2):
                at = (cc * 2 + yy) * mine
                X[k, at:at + mine, :] = G[k, cc, yy].reshape(mine, kw)
        for w in weights[k]:
            w.wait()
        for u in range(UC):
            cols = pl.ds(u * uw, uw)
            for i, v in enumerate((VG, VU)):
                value = jnp.dot(X[k], v[pl.ds(k * kw, kw), cols], preferred_element_type=F32)
                if k > 0:
                    value += A[i, :, cols]
                A[i, :, cols] = value
                if k == KC - 1:
                    SX[u, i] = value.astype(BF16)
            if k == KC - 1:
                send(SX.at[u], RX.at[u], xs.at[u], xr.at[u], x_peer)

    def await_x(u):
        pltpu.make_async_remote_copy(src_ref=SX.at[u], dst_ref=RX.at[u], send_sem=xs.at[u], recv_sem=xr.at[u],
                                     device_id=x_peer, device_id_type=MESH).wait_recv()

    def down(f, lo, hi):
        return lax.dot_general(H[:, lo:hi], VD[pl.ds(f * fw, fw), lo:hi], (((1,), (1,)), ((), ())),
                               preferred_element_type=F32).reshape(2, 2, mine, fw)

    def hidden(u):
        await_x(u)
        cols = pl.ds(u * uw, uw)
        gate = A[0, :, cols] + RX[u, 0].astype(F32)
        up = A[1, :, cols] + RX[u, 1].astype(F32)
        H[:, cols] = (gate / (1.0 + jnp.exp(-gate)) * up).astype(BF16)

    for u in range(UC - 1):
        hidden(u)
        for f in range(FC):
            if u == 0:
                downs[f].wait()
            value = down(f, u * uw, (u + 1) * uw)
            O[f] = O[f] + value if u else value
    hidden(UC - 1)
    if UC == 1:
        for f in range(FC):
            downs[f].wait()

    arrivals = {}

    def to_core(f):
        value = down(f, (UC - 1) * uw, UC * uw)
        O[f] = O[f] + value if UC > 1 else value
        send(O.at[f, 1 - c], RC.at[f], cs.at[f], cr.at[f], core_peer)
        arrivals["c", f] = sent[-1]

    def to_y(f):
        arrivals["c", f].wait_recv()
        SY[f] = (O[f, c, 1 - y] + RC[f, 1 - y]).astype(BF16)
        send(SY.at[f], RY.at[f], ys.at[f], yr.at[f], y_peer)
        arrivals["y", f] = sent[-1]

    def to_z(f):
        arrivals["y", f].wait_recv()
        total = (O[f, c, y] + RC[f, y] + RY[f].astype(F32)).reshape(R, T, fw)
        S2[f] = total
        SZ[f] = total.astype(BF16)
        for d in range(1, R):
            send(SZ.at[f, away[d]], RZ.at[f, d], zs.at[f, d], zr.at[f, d], z_peer[d])
            arrivals["z", f, d] = sent[-1]

    def finish(f):
        total = S2[f, r]
        for d in range(1, R):
            arrivals["z", f, d].wait_recv()
            total += RZ[f, d].astype(F32)
        out[:, pl.ds(f * fw, fw)] = total.astype(BF16)

    for f in range(FC):
        to_core(f)
        if f:
            to_y(f - 1)
    to_y(FC - 1)
    for f in range(FC):
        to_z(f)
    for f in range(FC):
        finish(f)
    for copy in sent:
        copy.wait_send()


def solution(mesh):
    n = mesh.shape["seq"]

    def on_device(tok, wg, wu, wd):
        T, K = tok.shape
        U = wg.shape[1]
        F = wd.shape[0]
        R = n // 4
        UC = max(1, U // 256)
        uw, kw, fw, rows, mine = U // UC, K // KC, F // FC, n * T, R * T
        dma = pltpu.SemaphoreType.DMA
        scratch = [
            pltpu.VMEM((KC, 2, 2, R, T, kw), BF16),
            pltpu.VMEM((KC, rows, kw), BF16),
            pltpu.VMEM((K, U), BF16),
            pltpu.VMEM((K, U), BF16),
            pltpu.VMEM((F, U), BF16),
            pltpu.VMEM((2, rows, U), F32),
            pltpu.VMEM((UC, 2, rows, uw), BF16),
            pltpu.VMEM((UC, 2, rows, uw), BF16),
            pltpu.VMEM((rows, U), BF16),
            pltpu.VMEM((FC, 2, 2, mine, fw), F32),
            pltpu.VMEM((FC, 2, mine, fw), F32),
            pltpu.VMEM((FC, mine, fw), BF16),
            pltpu.VMEM((FC, mine, fw), BF16),
            pltpu.VMEM((FC, R, T, fw), F32),
            pltpu.VMEM((FC, R, T, fw), BF16),
            pltpu.VMEM((FC, R, T, fw), BF16),
            dma((2, KC)), dma((FC,)), dma((KC,)),
            dma((KC, R)), dma((KC, R)), dma((KC, 2, R)), dma((KC, 2, 2, R)),
            dma((UC,)), dma((UC,)),
            dma((FC,)), dma((FC,)), dma((FC,)), dma((FC,)), dma((FC, R)), dma((FC, R)),
        ]
        return pl.pallas_call(
            functools.partial(ffn, R, T, UC),
            out_shape=jax.ShapeDtypeStruct((T, F), BF16),
            in_specs=[pl.BlockSpec(memory_space=pl.ANY)] * 4,
            out_specs=pl.BlockSpec(memory_space=pltpu.VMEM),
            scratch_shapes=scratch,
            compiler_params=pltpu.CompilerParams(
                collective_id=0, has_side_effects=True, vmem_limit_bytes=60 * 1024 * 1024
            ),
        )(tok, wg, wu, wd)

    return jax.shard_map(
        on_device,
        mesh=mesh,
        in_specs=(P("seq", "fsdp"), P("fsdp", "seq"), P("fsdp", "seq"), P("fsdp", "seq")),
        out_specs=P("seq", "fsdp"),
        check_vma=False,
    )
```
